256 devices in a mesh: px: 8 (over z_hi, x), py: 32 (over y, z_lo, core).
Axes of the slice: x: 4, y: 4, z: 8 (z_hi: 2, z_lo: 4; z = z_hi * 4 + z_lo), core: 2. Of those that a mesh axis runs over, the one named last changes fastest.
Arguments:
- populations: float32 [19, 2, 2048, 2048], P(None, None, ('py', 'px')), may hold values from 0.02 to 0.12
- pore: int32 [2, 2048, 2048], P(None, ('py', 'px')), may hold values 0 or 1
Outputs:
- flow: float32 [19, 2, 2048, 2048], P(None, None, 'py', 'px')
The draws below stay inside these ranges and needn't reach their ends.
All inputs are finite; a program needn't handle non-finite values. No bound on the sum of `pore` on one device may be relied on, other than what follows from the above.
Results may differ from the reference program's by a relative error of at most 0.0001.
Values sent between devices are 32-bit elements; how exact they have to be, the bound alone decides.
No kernel may reach another device: no remote copies, remote signals or barrier semaphores. Data moves between devices by JAX's collectives and lax.ppermute only.
A program may use at most 128 MiB of HBM per device.

```python
import jax
import jax.numpy as jnp

Q = 19
NZ = 2
STEPS = 2
NX = 2048
NY = 2048


def with_ends(values, key, least, largest):
    extent = values.shape
    index_at = [jax.random.randint(jax.random.fold_in(key, axis), (), 0, extent[axis]) for axis in range(len(extent))]
    values = values.at[tuple(index_at)].set(least)
    longest = extent.index(max(extent))
    index_at[longest] = (index_at[longest] + 1) % extent[longest]
    return values.at[tuple(index_at)].set(largest)


def block_levels(rng, dims, shards, low, top_value):
    factor_of = 1.0
    for dim, blocks in shards:
        heights = jax.random.uniform(jax.random.fold_in(jax.random.fold_in(rng, 6), dim), (blocks,), jnp.float32, low / len(shards), top_value / len(shards))
        factor_of = factor_of * jnp.repeat(jnp.exp(heights), dims[dim] // blocks).reshape((-1,) + (1,) * (len(dims) - 1 - dim))
    return factor_of


def setup_inputs(seed: int = 0) -> dict:
    streams_of = jax.random.split(jax.random.key(seed), 3)
    populations = jnp.clip(0.02 + 0.09999999776482582 * jax.random.uniform(streams_of[0], (Q, NZ, NY, NX), jnp.float32) ** block_levels(streams_of[0], (Q, NZ, NY, NX), ((2, 256),), -0.2, 0.2), 0.02, 0.12)
    pore = with_ends((jax.random.randint(streams_of[1], (NZ, NY, NX), 0, 4) < 3).astype(jnp.int32), jax.random.fold_in(streams_of[1], 1), 0, 1)
    return {"populations": populations, "pore": pore}


lattice_velocity = [(0, 0, 0), (1, 0, 0), (-1, 0, 0), (0, 1, 0), (0, -1, 0), (0, 0, 1), (0, 0, -1),
                    (1, 1, 0), (-1, -1, 0), (1, -1, 0), (-1, 1, 0), (1, 0, 1), (-1, 0, -1), (1, 0, -1),
                    (-1, 0, 1), (0, 1, 1), (0, -1, -1), (0, 1, -1), (0, -1, 1)]
lattice_weights = [1.0 / 3.0] + [1.0 / 18.0] * 6 + [1.0 / 36.0] * 12
opposite = [0, 2, 1, 4, 3, 6, 5, 8, 7, 10, 9, 12, 11, 14, 13, 16, 15, 18, 17]
relax_time = 0.8
body_force = 0.005


def moment(fields, column):
    total = jnp.zeros_like(fields[0])
    for slot in range(len(lattice_velocity)):
        vector = lattice_velocity[slot]
        if vector[column] != 0:
            total = total + float(vector[column]) * fields[slot]
    return total


def collide(fields, fluid):
    density = jnp.where(fluid > 0.5, jnp.sum(fields, axis=0), 1.0)
    vel_first = moment(fields, 0) / density
    vel_second = moment(fields, 1) / density
    vel_third = moment(fields, 2) / density + relax_time * body_force
    speed = vel_first * vel_first + vel_second * vel_second + vel_third * vel_third
    result = []
    for slot in range(len(lattice_velocity)):
        vector = lattice_velocity[slot]
        along = vector[0] * vel_first + vector[1] * vel_second + vector[2] * vel_third
        equil = lattice_weights[slot] * density * (1.0 + 3.0 * along + 4.5 * along * along - 1.5 * speed)
        result.append(fields[slot] - (fields[slot] - equil) / relax_time)
    return jnp.stack(result) * fluid[None]


def reference(populations, pore):
    fluid = pore.astype(jnp.float32)
    fields = populations
    for step in range(STEPS):
        post = collide(fields, fluid)
        result = []
        for slot in range(len(lattice_velocity)):
            vector = lattice_velocity[slot]
            source = jnp.roll(post[slot], (vector[2], vector[1], vector[0]), axis=(0, 1, 2))
            open_cell = jnp.roll(fluid, (vector[2], vector[1], vector[0]), axis=(0, 1, 2))
            result.append(jnp.where(open_cell > 0.5, source, post[opposite[slot]]))
        fields = jnp.stack(result) * fluid[None]
    return fields
```

```python
import functools

import jax
import jax.numpy as jnp
from jax import lax
from jax.experimental import pallas as pl
from jax.experimental.pallas import tpu as pltpu
from jax.sharding import PartitionSpec as P

lattice_velocity = [
    (0, 0, 0),
    (1, 0, 0),
    (-1, 0, 0),
    (0, 1, 0),
    (0, -1, 0),
    (0, 0, 1),
    (0, 0, -1),
    (1, 1, 0),
    (-1, -1, 0),
    (1, -1, 0),
    (-1, 1, 0),
    (1, 0, 1),
    (-1, 0, -1),
    (1, 0, -1),
    (-1, 0, 1),
    (0, 1, 1),
    (0, -1, -1),
    (0, 1, -1),
    (0, -1, 1),
]
opposite = [0, 2, 1, 4, 3, 6, 5, 8, 7, 10, 9, 12, 11, 14, 13, 16, 15, 18, 17]
relax_time = 0.8
body_force = 0.005
Q = 19
CH = Q + 1
TILES = 2 * CH + 1
SOLID = -1e30
F32 = jnp.float32


def row_masks():
    sub = lax.broadcasted_iota(jnp.int32, (8, 128), 0)
    middle = (sub >= 2) & (sub < 6)
    low = (sub & 2) == 0
    return middle, low


def pack_kernel(pop, pore, *outs):
    me = lax.axis_index("px")
    middle, _ = row_masks()
    lane = lax.broadcasted_iota(jnp.int32, (8, 128), 1)

    def load(channel, plane, tile):
        cols = pl.ds(pl.multiple_of(tile * 128, 128), 128)
        if channel < Q:
            return pop[channel, plane, :, cols]
        return pore[plane, :, cols].astype(F32)

    def put(out, tile, first, second):
        turned = pltpu.roll(second, 4, 0)
        edge_rows = jnp.where(middle, turned, first)
        inner_rows = jnp.where(middle, first, turned)
        if len(out) == 1:
            out[0][tile] = edge_rows
            out[0][TILES + tile] = inner_rows
        else:
            out[0][tile] = edge_rows
            out[1][tile] = inner_rows

    grouped = {k: (outs[k],) for k in range(4)}
    for k in range(4, 8):
        grouped[k] = (outs[k], outs[k + 4])
    for k in (4, 5, 6, 7, 1, 2, 3, 0):
        block = me ^ k
        for channel in range(CH):
            for half in range(2):
                tile = 2 * block + half
                put(
                    grouped[k],
                    2 * channel + half,
                    load(channel, 0, tile),
                    load(channel, 1, tile),
                )
        left = (2 * block + 15) & 15
        right = (2 * block + 2) & 15
        sides = []
        for plane in range(2):
            total = jnp.zeros((8, 128), F32)
            for channel in range(CH):
                ends = jnp.where(
                    lane < 64, load(channel, plane, right), load(channel, plane, left)
                )
                moved = pltpu.roll(ends, 2 + 4 * channel, 1)
                total = jnp.where((lane >> 2) == channel, moved, total)
            sides.append(total)
        put(grouped[k], 2 * CH, sides[0], sides[1])


def edge_kernel(*refs):
    tiles = refs[:8]
    down, up, first, last, sems = refs[8:]
    me = lax.axis_index("px")
    _, low = row_masks()
    for k in range(8):
        source = tiles[k].at[pl.ds(0, TILES)]

        @pl.when(me == k)
        def _():
            copy = pltpu.make_async_copy(source, first, sems.at[0])
            copy.start()
            copy.wait()

        @pl.when((me ^ 7) == k)
        def _():
            copy = pltpu.make_async_copy(source, last, sems.at[1])
            copy.start()
            copy.wait()

    for pair in range((TILES + 1) // 2):
        other = min(2 * pair + 1, TILES - 1)
        down[pair] = jnp.where(low, first[2 * pair], pltpu.roll(first[other], 2, 0))
        up[pair] = jnp.where(low, pltpu.roll(last[other], 6, 0), last[2 * pair])


def collide(f, fluid):
    sums = [f[2 * j + 1] + f[2 * j + 2] for j in range(9)]
    diffs = [f[2 * j + 1] - f[2 * j + 2] for j in range(9)]
    density = f[0] + ((sums[0] + sums[1]) + (sums[2] + sums[3])) + (
        (sums[4] + sums[5]) + (sums[6] + sums[7]) + sums[8]
    )
    density = jnp.where(fluid, density, 1.0)
    inverse = 1.0 / density
    vel = []
    for axis in range(3):
        total = None
        for j in range(9):
            sign = lattice_velocity[2 * j + 1][axis]
            if sign:
                if total is None:
                    total = diffs[j]
                elif sign > 0:
                    total = total + diffs[j]
                else:
                    total = total - diffs[j]
        vel.append(total * inverse)
    vel[2] = vel[2] + relax_time * body_force
    speed = vel[0] * vel[0] + vel[1] * vel[1] + vel[2] * vel[2]
    rate = 1.0 / relax_time
    keep = 1.0 - rate
    scaled = density * rate
    base = scaled - 1.5 * (scaled * speed)
    out = [keep * f[0] + (1.0 / 3.0) * base]
    parts = {}
    for share in (1.0 / 18.0, 1.0 / 36.0):
        parts[share] = (share * base, share * scaled)
    for j in range(9):
        vector = lattice_velocity[2 * j + 1]
        along = None
        for axis in range(3):
            if vector[axis]:
                if along is None:
                    along = vel[axis]
                elif vector[axis] > 0:
                    along = along + vel[axis]
                else:
                    along = along - vel[axis]
        rest, weight = parts[1.0 / 18.0 if j < 3 else 1.0 / 36.0]
        tilt = weight * along
        even = rest + 4.5 * (tilt * along)
        odd = 3.0 * tilt
        out.append(keep * f[2 * j + 1] + (even + odd))
        out.append(keep * f[2 * j + 2] + (even - odd))
    return out


def steps_kernel(*refs):
    wholes = refs[:4]
    edges = refs[4:8]
    inners = refs[8:12]
    down, up = refs[12:14]
    out = refs[14]
    post, post2, fluids, line = refs[15:]
    me = lax.axis_index("px")
    middle, low = row_masks()

    def store(rows, tile, plane, values, fluid):
        cols = pl.ds(128 * tile, 128)
        for slot in range(Q):
            post[slot, plane, rows, cols] = jnp.where(fluid, values[slot], SOLID)
        fluids[plane, rows, cols] = jnp.where(fluid, 1.0, 0.0)

    def first_step(read_edge, read_inner, rows):
        def unpack(tile, plane):
            a, b = read_edge(tile), read_inner(tile)
            if plane == 0:
                return jnp.where(middle, b, a)
            return pltpu.roll(jnp.where(middle, a, b), 4, 0)

        for plane in range(2):
            ends = unpack(2 * CH, plane)
            for tile in range(3):
                if tile < 2:
                    values = [unpack(2 * c + tile, plane) for c in range(CH)]
                else:
                    values = [pltpu.roll(ends, 126 - 4 * c, 1) for c in range(CH)]
                fluid = values[Q] > 0.5
                store(rows, tile, plane, collide(values[:Q], fluid), fluid)

    for k in range(8):
        strip = me ^ k
        rows = pl.ds(pl.multiple_of(8 + 8 * strip, 8), 8)
        if k < 4:
            first_step(
                lambda t, k=k: wholes[k][t], lambda t, k=k: wholes[k][TILES + t], rows
            )
        else:
            first_step(
                lambda t, k=k: edges[k - 4][t], lambda t, k=k: inners[k - 4][t], rows
            )

    def ring(tile):
        d, u = down[tile // 2], up[tile // 2]
        if tile % 2:
            d, u = pltpu.roll(d, 6, 0), pltpu.roll(u, 2, 0)
        return jnp.where(low, d, u)

    first_step(ring, ring, pl.ds(72, 8))

    def guards(array):
        for slot in range(Q):
            for plane in range(2):
                array[slot, plane, pl.ds(0, 8), :] = array[slot, plane, pl.ds(72, 8), :]
                array[slot, plane, pl.ds(80, 8), :] = array[slot, plane, pl.ds(8, 8), :]

    def streamed(array, slot, plane, row, open_here):
        vector = lattice_velocity[slot]
        here = array[opposite[slot], plane, pl.ds(row, 8), :]
        if slot == 0:
            return jnp.where(open_here, here, 0.0)
        from_plane = plane if vector[2] == 0 else 1 - plane
        source = array[slot, from_plane, pl.ds(row - vector[1], 8), :]
        if vector[0]:
            source = pltpu.roll(source, vector[0] % 384, 1)
        return jnp.where(open_here, jnp.where(source > 0.5 * SOLID, source, here), 0.0)

    guards(post)

    def second(plane, carry):
        for part in range(1, 10):
            row = 8 * part
            open_here = fluids[plane, pl.ds(row, 8), :] > 0.5
            for slot in range(Q):
                line[slot] = streamed(post, slot, plane, row, open_here)
            for tile in range(3):
                cols = pl.ds(128 * tile, 128)
                fluid = fluids[plane, pl.ds(row, 8), cols] > 0.5
                values = collide([line[slot, :, cols] for slot in range(Q)], fluid)
                for slot in range(Q):
                    post2[slot, plane, pl.ds(row, 8), cols] = jnp.where(
                        fluid, values[slot], SOLID
                    )
        return carry

    lax.fori_loop(0, 2, second, 0)
    guards(post2)

    def third(plane, carry):
        for part in range(1, 9):
            row = 8 * part
            open_here = fluids[plane, pl.ds(row, 8), :] > 0.5
            for slot in range(Q):
                result = streamed(post2, slot, plane, row, open_here)
                out[slot, plane, pl.ds(row - 8, 8), :] = result[:, :256]
        return carry

    lax.fori_loop(0, 2, third, 0)


def tiles_of(count):
    return jax.ShapeDtypeStruct((count, 8, 128), F32)


def vmem(count):
    return [pl.BlockSpec(memory_space=pltpu.VMEM)] * count


def body(populations, pore):
    planes, rows, width = populations.shape[1:]
    sent = pl.pallas_call(
        pack_kernel,
        out_shape=[tiles_of(2 * TILES)] * 4 + [tiles_of(TILES)] * 8,
        in_specs=vmem(2),
        out_specs=vmem(12),
        cost_estimate=pl.CostEstimate(
            flops=4_000_000, bytes_accessed=5_000_000, transcendentals=0
        ),
        name="pack",
    )(populations, pore)

    def trade(array, k):
        with jax.named_scope(f"trade{k}"):
            return lax.ppermute(array, "px", [(i, i ^ k) for i in range(8)])

    edges = [trade(sent[k], k) for k in range(4, 8)]
    wholes = [sent[0]] + [trade(sent[k], k) for k in range(1, 4)]
    inners = [trade(sent[k + 4], k) for k in range(4, 8)]

    pairs = (TILES + 1) // 2
    down, up = pl.pallas_call(
        edge_kernel,
        out_shape=[tiles_of(pairs)] * 2,
        in_specs=[pl.BlockSpec(memory_space=pl.ANY)] * 8,
        out_specs=vmem(2),
        scratch_shapes=[
            pltpu.VMEM((TILES, 8, 128), F32),
            pltpu.VMEM((TILES, 8, 128), F32),
            pltpu.SemaphoreType.DMA((2,)),
        ],
        cost_estimate=pl.CostEstimate(
            flops=500_000, bytes_accessed=500_000, transcendentals=0
        ),
        name="edge",
    )(*wholes, *edges)
    count = lax.axis_size("py")
    with jax.named_scope("below"):
        down = lax.ppermute(down, "py", [((i + 1) % count, i) for i in range(count)])
    with jax.named_scope("above"):
        up = lax.ppermute(up, "py", [(i, (i + 1) % count) for i in range(count)])

    return pl.pallas_call(
        steps_kernel,
        out_shape=jax.ShapeDtypeStruct((Q, planes, 64, 256), F32),
        in_specs=vmem(14),
        out_specs=pl.BlockSpec(memory_space=pltpu.VMEM),
        scratch_shapes=[
            pltpu.VMEM((Q, planes, 88, 384), F32),
            pltpu.VMEM((Q, planes, 88, 384), F32),
            pltpu.VMEM((planes, 88, 384), F32),
            pltpu.VMEM((Q, 8, 384), F32),
        ],
        cost_estimate=pl.CostEstimate(
            flops=40_000_000, bytes_accessed=6_000_000, transcendentals=0
        ),
        name="steps",
    )(*wholes, *edges, *inners, down, up)


def solution(mesh):
    return jax.shard_map(
        body,
        mesh=mesh,
        in_specs=(P(None, None, ("py", "px"), None), P(None, ("py", "px"), None)),
        out_specs=P(None, None, "py", "px"),
        check_vma=False,
    )
```

```python
import jax
import jax.numpy as jnp
from jax import lax
from jax.experimental import pallas as pl
from jax.experimental.pallas import tpu as pltpu
from jax.sharding import PartitionSpec as P


lattice_velocity = [
    (0, 0, 0),
    (1, 0, 0),
    (-1, 0, 0),
    (0, 1, 0),
    (0, -1, 0),
    (0, 0, 1),
    (0, 0, -1),
    (1, 1, 0),
    (-1, -1, 0),
    (1, -1, 0),
    (-1, 1, 0),
    (1, 0, 1),
    (-1, 0, -1),
    (1, 0, -1),
    (-1, 0, 1),
    (0, 1, 1),
    (0, -1, -1),
    (0, 1, -1),
    (0, -1, 1),
]
opposite = [0, 2, 1, 4, 3, 6, 5, 8, 7, 10, 9, 12, 11, 14, 13, 16, 15, 18, 17]
relax_time = 0.8
body_force = 0.005
Q = 19
TILES = 2 * Q + 1
SOLID = -1e30
F32 = jnp.float32


def row_masks():
    sub = lax.broadcasted_iota(jnp.int32, (8, 128), 0)
    middle = (sub >= 2) & (sub < 6)
    low = (sub & 2) == 0
    return middle, low


def pack_kernel(pop, pore, *refs, far):
    outs, (cells, voxels, post, sems) = refs[:-4], refs[-4:]
    me = lax.axis_index("px")
    half = (me >> 2) ^ far
    middle, _ = row_masks()
    lane = lax.broadcasted_iota(jnp.int32, (8, 128), 1)

    copies = []
    spans = [((8 * half + 15) & 15, 0, 1), ((8 * half + 8) & 15, 9, 1)]
    spans += [(8 * half + 2 * part, 1 + 2 * part, 2) for part in range(4)]
    for place, (start, local, size) in enumerate(spans):
        source = pl.ds(pl.multiple_of(128 * start, 128), 128 * size)
        target = pl.ds(128 * local, 128 * size)
        copies.append(
            pltpu.make_async_copy(
                pore.at[:, :, source], voxels.at[:, :, target], sems.at[1, place]
            )
        )
        copies.append(
            pltpu.make_async_copy(
                pop.at[:, :, :, source], cells.at[:, :, :, target], sems.at[0, place]
            )
        )
    for copy in copies:
        copy.start()
    for copy in copies:
        copy.wait()

    def first_step(tile, carry):
        cols = pl.ds(pl.multiple_of(128 * tile, 128), 128)
        for plane in range(2):
            fluid = voxels[plane, :, cols] > 0
            values = collide([cells[slot, plane, :, cols] for slot in range(Q)], fluid)
            for slot in range(Q):
                post[slot, plane, :, cols] = jnp.where(fluid, values[slot], 0.0)
        return carry

    lax.fori_loop(0, 10, first_step, 0)

    def load(slot, plane, tile):
        return post[slot, plane, :, pl.ds(pl.multiple_of(tile * 128, 128), 128)]

    for place in range(4):
        block = (me ^ place) & 3
        edge_out = outs[place].at[pl.ds(0, TILES)]
        inner_out = outs[4 + place] if far else outs[place].at[pl.ds(TILES, TILES)]

        def put(tile, first, second):
            turned = pltpu.roll(second, 4, 0)
            edge_out[tile] = jnp.where(middle, turned, first)
            inner_out[tile] = jnp.where(middle, first, turned)

        for slot in range(Q):
            for side in range(2):
                tile = 2 * block + 1 + side
                put(2 * slot + side, load(slot, 0, tile), load(slot, 1, tile))
        ends = []
        for plane in range(2):
            total = jnp.zeros((8, 128), F32)
            for slot in range(Q):
                both = jnp.where(
                    lane < 64,
                    load(slot, plane, 2 * block + 3),
                    load(slot, plane, 2 * block),
                )
                moved = pltpu.roll(both, 2 + 4 * slot, 1)
                total = jnp.where((lane >> 2) == slot, moved, total)
            ends.append(total)
        put(2 * Q, ends[0], ends[1])


def collide(f, fluid):
    sums = [f[2 * j + 1] + f[2 * j + 2] for j in range(9)]
    diffs = [f[2 * j + 1] - f[2 * j + 2] for j in range(9)]
    density = f[0] + ((sums[0] + sums[1]) + (sums[2] + sums[3])) + (
        (sums[4] + sums[5]) + (sums[6] + sums[7]) + sums[8]
    )
    density = jnp.where(fluid, density, 1.0)
    inverse = 1.0 / density
    vel = []
    for axis in range(3):
        total = None
        for j in range(9):
            sign = lattice_velocity[2 * j + 1][axis]
            if sign:
                if total is None:
                    total = diffs[j]
                elif sign > 0:
                    total = total + diffs[j]
                else:
                    total = total - diffs[j]
        vel.append(total * inverse)
    vel[2] = vel[2] + relax_time * body_force
    speed = vel[0] * vel[0] + vel[1] * vel[1] + vel[2] * vel[2]
    rate = 1.0 / relax_time
    keep = 1.0 - rate
    scaled = density * rate
    base = scaled - 1.5 * (scaled * speed)
    out = [keep * f[0] + (1.0 / 3.0) * base]
    parts = {}
    for share in (1.0 / 18.0, 1.0 / 36.0):
        parts[share] = (share * base, share * scaled)
    for j in range(9):
        vector = lattice_velocity[2 * j + 1]
        along = None
        for axis in range(3):
            if vector[axis]:
                if along is None:
                    along = vel[axis]
                elif vector[axis] > 0:
                    along = along + vel[axis]
                else:
                    along = along - vel[axis]
        rest, weight = parts[1.0 / 18.0 if j < 3 else 1.0 / 36.0]
        tilt = weight * along
        even = rest + 4.5 * (tilt * along)
        odd = 3.0 * tilt
        out.append(keep * f[2 * j + 1] + (even + odd))
        out.append(keep * f[2 * j + 2] + (even - odd))
    return out


def edge_kernel(*refs):
    tiles = refs[:8]
    down, up, first, last, sems = refs[8:]
    me = lax.axis_index("px")
    _, low = row_masks()
    for k in range(8):
        source = tiles[k].at[pl.ds(0, TILES)]

        @pl.when(me == k)
        def _():
            copy = pltpu.make_async_copy(source, first, sems.at[0])
            copy.start()
            copy.wait()

        @pl.when((me ^ 7) == k)
        def _():
            copy = pltpu.make_async_copy(source, last, sems.at[1])
            copy.start()
            copy.wait()

    for pair in range((TILES + 1) // 2):
        other = min(2 * pair + 1, TILES - 1)
        down[pair] = jnp.where(low, first[2 * pair], pltpu.roll(first[other], 2, 0))
        up[pair] = jnp.where(low, pltpu.roll(last[other], 6, 0), last[2 * pair])


def rows_of(part):
    return pl.ds(pl.multiple_of(8 * part, 8), 8)


def unpack(post, read_edge, read_inner, part):
    middle, _ = row_masks()

    def join(tile, plane):
        a, b = read_edge(tile), read_inner(tile)
        if plane == 0:
            return jnp.where(middle, b, a)
        return pltpu.roll(jnp.where(middle, a, b), 4, 0)

    for plane in range(2):
        ends = join(2 * Q, plane)
        for tile in range(3):
            if tile < 2:
                values = [join(2 * slot + tile, plane) for slot in range(Q)]
            else:
                values = [pltpu.roll(ends, 126 - 4 * slot, 1) for slot in range(Q)]
            density = values[0]
            for value in values[1:]:
                density = density + value
            for slot in range(Q):
                post[slot, plane, rows_of(part), pl.ds(128 * tile, 128)] = jnp.where(
                    density > 0.0, values[slot], SOLID
                )


def streamed(array, slot, plane, part, open_here):
    sub = lax.broadcasted_iota(jnp.int32, (8, 384), 0)
    vector = lattice_velocity[slot]
    here = array[opposite[slot], plane, rows_of(part), :]
    if slot == 0:
        return jnp.where(open_here, here, 0.0)
    origin = plane if vector[2] == 0 else 1 - plane
    source = array[slot, origin, rows_of(part), :]
    if vector[1] == 1:
        beyond = array[slot, origin, rows_of(lax.rem(part + 8, 9)), :]
        source = pltpu.roll(jnp.where(sub == 7, beyond, source), 1, 0)
    elif vector[1] == -1:
        beyond = array[slot, origin, rows_of(lax.rem(part + 1, 9)), :]
        source = pltpu.roll(jnp.where(sub == 0, beyond, source), 7, 0)
    if vector[0]:
        source = pltpu.roll(source, vector[0] % 384, 1)
    return jnp.where(open_here, jnp.where(source > 0.5 * SOLID, source, here), 0.0)


def second_step(post, post2, line, part):
    for plane in range(2):
        open_here = post[0, plane, rows_of(part), :] > 0.5 * SOLID
        for slot in range(Q):
            line[slot, plane] = streamed(post, slot, plane, part, open_here)
        for tile in range(3):
            cols = pl.ds(128 * tile, 128)
            fluid = post[0, plane, rows_of(part), cols] > 0.5 * SOLID
            values = collide([line[slot, plane, :, cols] for slot in range(Q)], fluid)
            for slot in range(Q):
                post2[slot, plane, rows_of(part), cols] = jnp.where(
                    fluid, values[slot], SOLID
                )


def finish(post2, stage, flow, sem, part):
    for plane in range(2):
        open_here = post2[0, plane, rows_of(part), :] > 0.5 * SOLID
        for slot in range(Q):
            result = streamed(post2, slot, plane, part, open_here)
            stage[slot, plane, rows_of(part), :] = result[:, :256]
    part_copy(stage, flow, sem, part).start()


def part_copy(stage, flow, sem, part):
    return pltpu.make_async_copy(
        stage.at[:, :, rows_of(part), :], flow.at[:, :, rows_of(part), :], sem.at[part]
    )


def finish_all(post2, stage, flow, sem, offsets, strip):
    for offset in offsets:
        part = lax.rem(strip + offset, 9)

        @pl.when(part < 8)
        def _():
            finish(post2, stage, flow, sem, part)

    for offset in offsets:
        part = lax.rem(strip + offset, 9)

        @pl.when(part < 8)
        def _():
            part_copy(stage, flow, sem, part).wait()


def early_kernel(*refs):
    wholes, edges, inners = refs[:4], refs[4:6], refs[6:8]
    down, up = refs[8:10]
    post, post2, flow, line, stage, sem = refs[10:]
    me = lax.axis_index("px")
    _, low = row_masks()
    for k in range(4):
        unpack(
            post, lambda t, k=k: wholes[k][t], lambda t, k=k: wholes[k][TILES + t], me ^ k
        )
    for k in range(2):
        unpack(
            post, lambda t, k=k: edges[k][t], lambda t, k=k: inners[k][t], me ^ (4 + k)
        )

    def ring(tile):
        d, u = down[tile // 2], up[tile // 2]
        if tile % 2:
            d, u = pltpu.roll(d, 6, 0), pltpu.roll(u, 2, 0)
        return jnp.where(low, d, u)

    unpack(post, ring, ring, 8)
    strip = (me ^ 6) & 6

    def step(offset, carry):
        second_step(post, post2, line, lax.rem(strip + offset, 9))
        return carry

    lax.fori_loop(3, 8, step, 0)
    finish_all(post2, stage, flow, sem, (4, 5, 6), strip)


def late_kernel(*refs):
    edges, inners = refs[:2], refs[2:4]
    post, post2, flow, line, stage, sem = refs[7:]
    me = lax.axis_index("px")
    for k in range(2):
        unpack(
            post, lambda t, k=k: edges[k][t], lambda t, k=k: inners[k][t], me ^ (6 + k)
        )
    strip = (me ^ 6) & 6

    def step(offset, carry):
        second_step(post, post2, line, lax.rem(strip + 8 + offset, 9))
        return carry

    lax.fori_loop(0, 4, step, 0)
    finish_all(post2, stage, flow, sem, (7, 8, 0, 1, 2, 3), strip)


def tiles_of(count):
    return jax.ShapeDtypeStruct((count, 8, 128), F32)


def vmem(count):
    return [pl.BlockSpec(memory_space=pltpu.VMEM)] * count


def anywhere(count):
    return [pl.BlockSpec(memory_space=pl.ANY)] * count


def grant(mebibytes):
    return pltpu.CompilerParams(vmem_limit_bytes=mebibytes * 2**20)


def cost(flops):
    return pl.CostEstimate(flops=flops, bytes_accessed=2_000_000, transcendentals=0)


def step_pair(populations, pore):
    planes, rows, width = populations.shape[1:]
    wide = width // 2 + 256

    def pack(far):
        shapes = [tiles_of(TILES)] * 8 if far else [tiles_of(2 * TILES)] * 4
        return pl.pallas_call(
            lambda *refs: pack_kernel(*refs, far=far),
            out_shape=shapes,
            in_specs=[pl.BlockSpec(memory_space=pltpu.HBM)] * 2,
            out_specs=vmem(len(shapes)),
            scratch_shapes=[
                pltpu.VMEM((Q, planes, rows, wide), F32),
                pltpu.VMEM((planes, rows, wide), jnp.int32),
                pltpu.VMEM((Q, planes, rows, wide), F32),
                pltpu.SemaphoreType.DMA((2, 6)),
            ],
            compiler_params=grant(16),
            cost_estimate=cost(4_000_000),
            name="pack_far" if far else "pack_near",
        )(populations, pore)

    def trade(array, k):
        return lax.ppermute(array, "px", [(i, i ^ k) for i in range(8)])

    far = pack(1)
    near = pack(0)
    edges = [trade(far[k], 4 + k) for k in range(4)]
    wholes = [near[0]] + [trade(near[k], k) for k in range(1, 4)]
    inners = [trade(far[4 + k], 4 + k) for k in range(4)]

    pairs = (TILES + 1) // 2
    down, up = pl.pallas_call(
        edge_kernel,
        out_shape=[tiles_of(pairs)] * 2,
        in_specs=anywhere(8),
        out_specs=vmem(2),
        scratch_shapes=[
            pltpu.VMEM((TILES, 8, 128), F32),
            pltpu.VMEM((TILES, 8, 128), F32),
            pltpu.SemaphoreType.DMA((2,)),
        ],
        compiler_params=grant(4),
        cost_estimate=cost(500_000),
        name="edge",
    )(*wholes, *edges)
    count = lax.axis_size("py")
    down = lax.ppermute(down, "py", [((i + 1) % count, i) for i in range(count)])
    up = lax.ppermute(up, "py", [(i, (i + 1) % count) for i in range(count)])

    ring = jax.ShapeDtypeStruct((Q, planes, 72, 384), F32)
    result = jax.ShapeDtypeStruct((Q, planes, 64, 256), F32)
    scratch = [
        pltpu.VMEM((Q, planes, 8, 384), F32),
        pltpu.VMEM((Q, planes, 64, 256), F32),
        pltpu.SemaphoreType.DMA((9,)),
    ]
    post, post2, flow = pl.pallas_call(
        early_kernel,
        out_shape=[ring, ring, result],
        in_specs=vmem(10),
        out_specs=vmem(2) + anywhere(1),
        scratch_shapes=scratch,
        compiler_params=grant(24),
        cost_estimate=cost(40_000_000),
        name="early",
    )(*wholes, *edges[:2], *inners[:2], down, up)
    return pl.pallas_call(
        late_kernel,
        out_shape=[ring, ring, result],
        in_specs=vmem(6) + anywhere(1),
        out_specs=vmem(2) + anywhere(1),
        scratch_shapes=scratch,
        input_output_aliases={4: 0, 5: 1, 6: 2},
        compiler_params=grant(24),
        cost_estimate=cost(10_000_000),
        name="late",
    )(*edges[2:], *inners[2:], post, post2, flow)[2]


def solution(mesh):
    return jax.shard_map(
        step_pair,
        mesh=mesh,
        in_specs=(P(None, None, ("py", "px"), None), P(None, ("py", "px"), None)),
        out_specs=P(None, None, "py", "px"),
        check_vma=False,
    )
```

```python
import jax
import jax.numpy as jnp
from jax import lax
from jax.experimental import pallas as pl
from jax.experimental.pallas import tpu as pltpu
from jax.sharding import PartitionSpec as P


lattice_velocity = [
    (0, 0, 0),
    (1, 0, 0),
    (-1, 0, 0),
    (0, 1, 0),
    (0, -1, 0),
    (0, 0, 1),
    (0, 0, -1),
    (1, 1, 0),
    (-1, -1, 0),
    (1, -1, 0),
    (-1, 1, 0),
    (1, 0, 1),
    (-1, 0, -1),
    (1, 0, -1),
    (-1, 0, 1),
    (0, 1, 1),
    (0, -1, -1),
    (0, 1, -1),
    (0, -1, 1),
]
opposite = [0, 2, 1, 4, 3, 6, 5, 8, 7, 10, 9, 12, 11, 14, 13, 16, 15, 18, 17]
relax_time = 0.8
body_force = 0.005
Q = 19
TILES = 4 * Q + 1
FRONT = 26
BACK = TILES - FRONT
SOLID = -1e30
F32 = jnp.float32


def plan(me, half):
    place = me & 3
    second = place ^ (3 * half)
    second = jnp.where(second == 0, 1, second)
    third = lax.rem(second, 3) + 1
    return second, third, lax.rem(third, 3) + 1


def halo_lanes():
    places, lane = [], 0
    for slot in range(Q + 1):
        along_x = lattice_velocity[slot][0] if slot < Q else None
        first = 0 if along_x in (1, None) else 1
        last = 4 if along_x in (-1, None) else 3
        places.append((lane, first, last - first))
        lane += last - first
    return places, lane


def halo_rows(toward):
    items = [("near", tile) for tile in range(TILES)]
    for slot in range(Q):
        if lattice_velocity[slot][1] == toward:
            items += [("far", 4 * slot + part) for part in range(4)]
    items.append(("far", 4 * Q))
    items += [("density", part) for part in range(4)]
    return {item: divmod(index, 8) for index, item in enumerate(items)}


HALO_TILES = -(-len(halo_rows(1)) // 8)


def pack_kernel(pop, pore, *refs, far):
    outs, (post, cells, voxels, sems) = refs[:-4], refs[-4:]
    me = lax.axis_index("px")
    half = (me >> 2) ^ far
    lane = lax.broadcasted_iota(jnp.int32, (8, 128), 1)
    places, span = halo_lanes()

    def first_step(target, read, fluid_of):
        cols = pl.ds(pl.multiple_of(128 * target, 128), 128)
        for plane in range(2):
            fluid = fluid_of(plane)
            values = collide([read(slot, plane) for slot in range(Q)], fluid)
            for slot in range(Q):
                post[slot, plane, :, cols] = jnp.where(fluid, values[slot], 0.0)

    spans = [(8 * half + 2 * part, 1 + 2 * part, 2) for part in range(4)]
    spans += [((8 * half + 15) & 15, 0, 1), ((8 * half + 8) & 15, 9, 1)]
    copies = []
    for place, (start, local, size) in enumerate(spans):
        source = pl.ds(pl.multiple_of(128 * start, 128), 128 * size)
        target = pl.ds(128 * local, 128 * size)
        copies.append(
            (
                pltpu.make_async_copy(
                    pore.at[:, :, source], voxels.at[:, :, target], sems.at[1, place]
                ),
                pltpu.make_async_copy(
                    pop.at[:, :, :, source], cells.at[:, :, :, target], sems.at[0, place]
                ),
            )
        )
    for pair in copies:
        for copy in pair:
            copy.start()
    for pair, (_, local, size) in zip(copies, spans):
        for copy in pair:
            copy.wait()
        for tile in range(local, local + size):
            cols = pl.ds(128 * tile, 128)
            first_step(
                tile,
                lambda slot, plane: cells[slot, plane, :, cols],
                lambda plane: voxels[plane, :, cols] > 0,
            )

    def load(slot, plane, tile):
        return post[slot, plane, :, pl.ds(pl.multiple_of(tile * 128, 128), 128)]

    for place in range(4):
        block = (me ^ place) & 3

        def put(tile, value):
            if place == 0 or not far:
                outs[place][tile] = value
            elif tile < FRONT:
                outs[place][tile] = value
            else:
                outs[3 + place][tile - FRONT] = value

        for slot in range(Q):
            for plane in range(2):
                for side in range(2):
                    put(
                        4 * slot + 2 * plane + side,
                        load(slot, plane, 2 * block + 1 + side),
                    )
        ends = []
        for plane in range(2):
            total = jnp.zeros((8, 128), F32)
            density = jnp.zeros((8, 128), F32)
            for slot in range(Q + 1):
                if slot < Q:
                    both = jnp.where(
                        lane < 64,
                        load(slot, plane, 2 * block + 3),
                        load(slot, plane, 2 * block),
                    )
                    density = density + both
                else:
                    both = density
                start, first, count = places[slot]
                moved = pltpu.roll(both, (2 + start - first) % 128, 1)
                total = jnp.where((lane >= start) & (lane < start + count), moved, total)
            ends.append(total)
        put(4 * Q, jnp.where(lane < span, ends[0], pltpu.roll(ends[1], span, 1)))


def pick_second(first, other, last, out):
    me = lax.axis_index("px")
    wanted = plan(me, me >> 2)[0]
    for k, source in enumerate((first, other, last), 1):

        @pl.when(wanted == k)
        def _():
            out[...] = source[...]


def pick_rest(*refs):
    tops, bottoms, outs = refs[:3], refs[3:6], refs[6:]
    me = lax.axis_index("px")
    for round_, wanted in enumerate(plan(me, me >> 2)):
        for k in range(1, 4):

            @pl.when(wanted == k)
            def _():
                if round_ == 0:
                    outs[0][...] = bottoms[k - 1][...]
                else:
                    outs[round_][pl.ds(0, FRONT)] = tops[k - 1][...]
                    outs[round_][pl.ds(FRONT, BACK)] = bottoms[k - 1][...]


def edge_kernel(*refs):
    nears, own, top, bottom = refs[:4], refs[4], refs[5], refs[6]
    down, up, first, last = refs[7:]
    me = lax.axis_index("px")
    half, place = me >> 2, me & 3
    for mine in range(2):
        near_to, far_to = (first, last) if mine == 0 else (last, first)
        for k in range(4):

            @pl.when((half == mine) & ((place ^ (3 * mine)) == k))
            def _():
                near_to[...] = nears[k][...]

        edge_place = 3 * (1 - mine)

        @pl.when((half == mine) & (place == edge_place))
        def _():
            far_to[...] = own[...]

        @pl.when((half == mine) & (place != edge_place))
        def _():
            far_to[pl.ds(0, FRONT)] = top[...]
            far_to[pl.ds(FRONT, BACK)] = bottom[...]

    sub = lax.broadcasted_iota(jnp.int32, (8, 128), 0)
    for out, strip, toward in ((down, first, -1), (up, last, 1)):
        near_row, far_row = (0, 1) if toward == -1 else (7, 6)
        packed = [jnp.zeros((8, 128), F32)] * HALO_TILES
        for (kind, tile), (group, row) in halo_rows(toward).items():
            if kind == "density":
                value = strip[tile]
                for slot in range(1, Q):
                    value = value + strip[4 * slot + tile]
            else:
                value = strip[tile]
            origin = near_row if kind == "near" else far_row
            packed[group] = jnp.where(sub == row, turned(value, row - origin), packed[group])
        for group in range(HALO_TILES):
            out[group] = packed[group]


def turned(value, rows):
    return pltpu.roll(value, rows % 8, 0) if rows % 8 else value


def collide(f, fluid):
    sums = [f[2 * j + 1] + f[2 * j + 2] for j in range(9)]
    diffs = [f[2 * j + 1] - f[2 * j + 2] for j in range(9)]
    density = f[0] + ((sums[0] + sums[1]) + (sums[2] + sums[3])) + (
        (sums[4] + sums[5]) + (sums[6] + sums[7]) + sums[8]
    )
    density = jnp.where(fluid, density, 1.0)
    inverse = 1.0 / density
    vel = []
    for axis in range(3):
        total = None
        for j in range(9):
            sign = lattice_velocity[2 * j + 1][axis]
            if sign:
                if total is None:
                    total = diffs[j]
                elif sign > 0:
                    total = total + diffs[j]
                else:
                    total = total - diffs[j]
        vel.append(total * inverse)
    vel[2] = vel[2] + relax_time * body_force
    speed = vel[0] * vel[0] + vel[1] * vel[1] + vel[2] * vel[2]
    rate = 1.0 / relax_time
    keep = 1.0 - rate
    scaled = density * rate
    base = scaled - 1.5 * (scaled * speed)
    out = [keep * f[0] + (1.0 / 3.0) * base]
    parts = {}
    for share in (1.0 / 18.0, 1.0 / 36.0):
        parts[share] = (share * base, share * scaled)
    for j in range(9):
        vector = lattice_velocity[2 * j + 1]
        along = None
        for axis in range(3):
            if vector[axis]:
                if along is None:
                    along = vel[axis]
                elif vector[axis] > 0:
                    along = along + vel[axis]
                else:
                    along = along - vel[axis]
        rest, weight = parts[1.0 / 18.0 if j < 3 else 1.0 / 36.0]
        tilt = weight * along
        even = rest + 4.5 * (tilt * along)
        odd = 3.0 * tilt
        out.append(keep * f[2 * j + 1] + (even + odd))
        out.append(keep * f[2 * j + 2] + (even - odd))
    return out


def rows_of(part):
    return pl.ds(pl.multiple_of(8 * part, 8), 8)


def unpack(post, read, part, outer_density=None):
    places, span = halo_lanes()
    sub = lax.broadcasted_iota(jnp.int32, (8, 128), 0)
    packed = read(4 * Q)
    for plane in range(2):
        ends = pltpu.roll(packed, 128 - span, 1) if plane else packed
        for tile in range(3):
            if tile < 2:
                values = [read(4 * slot + 2 * plane + tile) for slot in range(Q)]
                density = values[0]
                for value in values[1:]:
                    density = density + value
                if outer_density is not None:
                    density = jnp.where(
                        (sub == 1) | (sub == 6), outer_density(2 * plane + tile), density
                    )
            else:
                values = [
                    pltpu.roll(ends, (first - 2 - start) % 128, 1)
                    for start, first, _ in places
                ]
                density = values.pop()
            for slot in range(Q):
                post[slot, plane, rows_of(part), pl.ds(128 * tile, 128)] = jnp.where(
                    density > 0.0, values[slot], SOLID
                )


def streamed(array, slot, plane, part, open_here):
    sub = lax.broadcasted_iota(jnp.int32, (8, 384), 0)
    vector = lattice_velocity[slot]
    here = array[opposite[slot], plane, rows_of(part), :]
    if slot == 0:
        return jnp.where(open_here, here, 0.0)
    origin = plane if vector[2] == 0 else 1 - plane
    source = array[slot, origin, rows_of(part), :]
    if vector[1] == 1:
        beyond = array[slot, origin, rows_of(lax.rem(part + 8, 9)), :]
        source = pltpu.roll(jnp.where(sub == 7, beyond, source), 1, 0)
    elif vector[1] == -1:
        beyond = array[slot, origin, rows_of(lax.rem(part + 1, 9)), :]
        source = pltpu.roll(jnp.where(sub == 0, beyond, source), 7, 0)
    if vector[0]:
        source = pltpu.roll(source, vector[0] % 384, 1)
    return jnp.where(open_here, jnp.where(source > 0.5 * SOLID, source, here), 0.0)


def second_step(post, post2, line, part):
    for plane in range(2):
        open_here = post[0, plane, rows_of(part), :] > 0.5 * SOLID
        for slot in range(Q):
            line[slot, plane] = streamed(post, slot, plane, part, open_here)
        for tile in range(3):
            cols = pl.ds(128 * tile, 128)
            fluid = post[0, plane, rows_of(part), cols] > 0.5 * SOLID
            values = collide([line[slot, plane, :, cols] for slot in range(Q)], fluid)
            for slot in range(Q):
                post2[slot, plane, rows_of(part), cols] = jnp.where(
                    fluid, values[slot], SOLID
                )


def finish(post2, stage, flow, sem, part):
    for plane in range(2):
        open_here = post2[0, plane, rows_of(part), :] > 0.5 * SOLID
        for slot in range(Q):
            result = streamed(post2, slot, plane, part, open_here)
            stage[slot, plane, rows_of(part), :] = result[:, :256]
    part_copy(stage, flow, sem, part).start()


def part_copy(stage, flow, sem, part):
    return pltpu.make_async_copy(
        stage.at[:, :, rows_of(part), :], flow.at[:, :, rows_of(part), :], sem.at[part]
    )


def finish_all(post2, stage, flow, sem, offsets, strip):
    for offset in offsets:
        part = lax.rem(strip + offset, 9)

        @pl.when(part < 8)
        def _():
            finish(post2, stage, flow, sem, part)

    for offset in offsets:
        part = lax.rem(strip + offset, 9)

        @pl.when(part < 8)
        def _():
            part_copy(stage, flow, sem, part).wait()


def early_kernel(*refs):
    nears, own, top, bottom, third = refs[:4], refs[4], refs[5], refs[6], refs[7]
    down, up = refs[8:10]
    post, post2, flow, line, stage, sem = refs[10:]
    me = lax.axis_index("px")
    half, place = me >> 2, me & 3
    second_k, third_k, last_k = plan(me, 1 - half)
    base = 4 * (1 - half)
    for k in range(4):
        unpack(post, lambda t, k=k: nears[k][t], me ^ k)
    unpack(post, lambda t: own[t], base + place)
    unpack(
        post,
        lambda t: top[t] if t < FRONT else bottom[t - FRONT],
        base + (place ^ second_k),
    )
    unpack(post, lambda t: third[t], base + (place ^ third_k))
    sub = lax.broadcasted_iota(jnp.int32, (8, 128), 0)

    below, above = halo_rows(-1), halo_rows(1)

    def row_from(array, where, row):
        group, origin = where
        return turned(array[group], row - origin)

    def ring(tile):
        value = jnp.where(
            sub == 0,
            row_from(down, below["near", tile], 0),
            row_from(up, above["near", tile], 7),
        )
        if ("far", tile) in below:
            value = jnp.where(sub == 1, row_from(down, below["far", tile], 1), value)
        if ("far", tile) in above:
            value = jnp.where(sub == 6, row_from(up, above["far", tile], 6), value)
        return value

    def ring_density(tile):
        return jnp.where(
            sub == 1,
            row_from(down, below["density", tile], 1),
            row_from(up, above["density", tile], 6),
        )

    unpack(post, ring, 8, ring_density)
    strip = base + (place ^ last_k)

    def step(offset, carry):
        second_step(post, post2, line, lax.rem(strip + offset, 9))
        return carry

    lax.fori_loop(2, 8, step, 0)
    finish_all(post2, stage, flow, sem, (3, 4, 5, 6), strip)


def late_kernel(last, post_in, post2_in, flow_in, post, post2, flow, line, stage, sem):
    me = lax.axis_index("px")
    half, place = me >> 2, me & 3
    strip = 4 * (1 - half) + (place ^ plan(me, 1 - half)[2])
    unpack(post, lambda t: last[t], strip)

    def step(offset, carry):
        second_step(post, post2, line, lax.rem(strip + 8 + offset, 9))
        return carry

    lax.fori_loop(0, 3, step, 0)
    finish_all(post2, stage, flow, sem, (7, 8, 0, 1, 2), strip)


def tiles_of(count):
    return jax.ShapeDtypeStruct((count, 8, 128), F32)


def vmem(count):
    return [pl.BlockSpec(memory_space=pltpu.VMEM)] * count


def anywhere(count):
    return [pl.BlockSpec(memory_space=pl.ANY)] * count


def grant(mebibytes):
    return pltpu.CompilerParams(vmem_limit_bytes=mebibytes * 2**20)


def cost(flops):
    return pl.CostEstimate(flops=flops, bytes_accessed=2_000_000, transcendentals=0)


def step_pair(populations, pore):
    planes, rows, width = populations.shape[1:]
    wide = width // 2 + 256

    def call(
        kernel, shapes, operands, grant_mib, scratch=(), flops=300_000, specs=None
    ):
        return pl.pallas_call(
            kernel,
            out_shape=shapes,
            in_specs=specs or vmem(len(operands)),
            out_specs=vmem(len(shapes)),
            scratch_shapes=list(scratch),
            compiler_params=grant(grant_mib),
            cost_estimate=cost(flops),
        )(*operands)

    def pack(far):
        whole = tiles_of(TILES)
        scratch = [pltpu.VMEM((Q, planes, rows, wide), F32)]
        scratch += [
            pltpu.VMEM((Q, planes, rows, wide), F32),
            pltpu.VMEM((planes, rows, wide), jnp.int32),
            pltpu.SemaphoreType.DMA((2, 6)),
        ]
        return call(
            lambda *refs: pack_kernel(*refs, far=far),
            [whole] + [tiles_of(FRONT)] * 3 + [tiles_of(BACK)] * 3 if far else [whole] * 4,
            (populations, pore),
            52,
            scratch=scratch,
            flops=4_000_000,
            specs=anywhere(2),
        )

    def trade(array, k):
        return lax.ppermute(array, "px", [(i, i ^ k) for i in range(8)])

    far = pack(1)
    near = pack(0)
    own = trade(far[0], 4)
    tops = [trade(far[k], k) for k in range(1, 4)]
    bottoms = [trade(far[3 + k], k) for k in range(1, 4)]
    (second,) = call(pick_second, [tiles_of(FRONT)], tops, 2)
    rest = call(
        pick_rest, [tiles_of(BACK), tiles_of(TILES), tiles_of(TILES)], tops + bottoms, 4
    )
    second_top = trade(second, 4)
    nears = [near[0]] + [trade(near[k], k) for k in range(1, 4)]
    second_bottom = trade(rest[0], 4)
    third = trade(rest[1], 4)
    fourth = trade(rest[2], 4)

    arrived = nears + [own, second_top, second_bottom]
    down, up = call(
        edge_kernel,
        [tiles_of(HALO_TILES)] * 2,
        arrived,
        4,
        scratch=[pltpu.VMEM((TILES, 8, 128), F32)] * 2,
        flops=500_000,
    )
    count = lax.axis_size("py")
    down = lax.ppermute(down, "py", [((i + 1) % count, i) for i in range(count)])
    up = lax.ppermute(up, "py", [(i, (i + 1) % count) for i in range(count)])

    ring = jax.ShapeDtypeStruct((Q, planes, 72, 384), F32)
    result = jax.ShapeDtypeStruct((Q, planes, 64, 256), F32)
    scratch = [
        pltpu.VMEM((Q, planes, 8, 384), F32),
        pltpu.VMEM((Q, planes, 64, 256), F32),
        pltpu.SemaphoreType.DMA((9,)),
    ]
    post, post2, flow = pl.pallas_call(
        early_kernel,
        out_shape=[ring, ring, result],
        in_specs=vmem(10),
        out_specs=vmem(2) + anywhere(1),
        scratch_shapes=scratch,
        compiler_params=grant(24),
        cost_estimate=cost(40_000_000),
        name="early",
    )(*arrived, third, down, up)
    return pl.pallas_call(
        late_kernel,
        out_shape=[ring, ring, result],
        in_specs=vmem(3) + anywhere(1),
        out_specs=vmem(2) + anywhere(1),
        scratch_shapes=scratch,
        input_output_aliases={1: 0, 2: 1, 3: 2},
        compiler_params=grant(24),
        cost_estimate=cost(10_000_000),
        name="late",
    )(fourth, post, post2, flow)[2]


def solution(mesh):
    return jax.shard_map(
        step_pair,
        mesh=mesh,
        in_specs=(P(None, None, ("py", "px"), None), P(None, ("py", "px"), None)),
        out_specs=P(None, None, "py", "px"),
        check_vma=False,
    )
```

```python
import jax
import jax.numpy as jnp
from jax import lax
from jax.experimental import pallas as pl
from jax.experimental.pallas import tpu as pltpu
from jax.sharding import PartitionSpec as P


lattice_velocity = [
    (0, 0, 0),
    (1, 0, 0),
    (-1, 0, 0),
    (0, 1, 0),
    (0, -1, 0),
    (0, 0, 1),
    (0, 0, -1),
    (1, 1, 0),
    (-1, -1, 0),
    (1, -1, 0),
    (-1, 1, 0),
    (1, 0, 1),
    (-1, 0, -1),
    (1, 0, -1),
    (-1, 0, 1),
    (0, 1, 1),
    (0, -1, -1),
    (0, 1, -1),
    (0, -1, 1),
]
opposite = [0, 2, 1, 4, 3, 6, 5, 8, 7, 10, 9, 12, 11, 14, 13, 16, 15, 18, 17]
relax_time = 0.8
body_force = 0.005
Q = 19
TILES = 4 * Q + 1
FRONT = 26
BACK = TILES - FRONT
SOLID = -1e30
F32 = jnp.float32


def plan(me, half):
    place = me & 3
    second = place ^ (3 * half)
    second = jnp.where(second == 0, 1, second)
    third = lax.rem(second, 3) + 1
    return second, third, lax.rem(third, 3) + 1


def halo_lanes():
    places, lane = [], 0
    for slot in range(Q + 1):
        along_x = lattice_velocity[slot][0] if slot < Q else None
        first = 0 if along_x in (1, None) else 1
        last = 4 if along_x in (-1, None) else 3
        places.append((lane, first, last - first))
        lane += last - first
    return places, lane


def halo_rows(toward):
    items = [("near", tile) for tile in range(TILES)]
    for slot in range(Q):
        if lattice_velocity[slot][1] == toward:
            items += [("far", 4 * slot + part) for part in range(4)]
    items.append(("far", 4 * Q))
    items += [("density", part) for part in range(4)]
    return {item: divmod(index, 8) for index, item in enumerate(items)}


HALO_TILES = -(-len(halo_rows(1)) // 8)


def pack_kernel(pop, pore, *refs, far):
    outs, (post, cells, voxels, sems) = refs[:-4], refs[-4:]
    me = lax.axis_index("px")
    half = (me >> 2) ^ far
    lane = lax.broadcasted_iota(jnp.int32, (8, 128), 1)
    places, span = halo_lanes()

    def first_step(target, read, fluid_of):
        cols = pl.ds(pl.multiple_of(128 * target, 128), 128)
        for plane in range(2):
            fluid = fluid_of(plane)
            values = collide([read(slot, plane) for slot in range(Q)], fluid)
            for slot in range(Q):
                post[slot, plane, :, cols] = jnp.where(fluid, values[slot], 0.0)

    spans = [(8 * half + 2 * part, 1 + 2 * part, 2) for part in range(4)]
    spans += [((8 * half + 15) & 15, 0, 1), ((8 * half + 8) & 15, 9, 1)]
    copies = []
    for place, (start, local, size) in enumerate(spans):
        source = pl.ds(pl.multiple_of(128 * start, 128), 128 * size)
        target = pl.ds(128 * local, 128 * size)
        copies.append(
            (
                pltpu.make_async_copy(
                    pore.at[:, :, source], voxels.at[:, :, target], sems.at[1, place]
                ),
                pltpu.make_async_copy(
                    pop.at[:, :, :, source], cells.at[:, :, :, target], sems.at[0, place]
                ),
            )
        )
    for pair in copies:
        for copy in pair:
            copy.start()
    for pair, (_, local, size) in zip(copies, spans):
        for copy in pair:
            copy.wait()
        for tile in range(local, local + size):
            cols = pl.ds(128 * tile, 128)
            first_step(
                tile,
                lambda slot, plane: cells[slot, plane, :, cols],
                lambda plane: voxels[plane, :, cols] > 0,
            )

    def load(slot, plane, tile):
        return post[slot, plane, :, pl.ds(pl.multiple_of(tile * 128, 128), 128)]

    for place in range(4):
        block = (me ^ place) & 3

        def put(tile, value):
            if place == 0 or not far:
                outs[place][tile] = value
            elif tile < FRONT:
                outs[place][tile] = value
            else:
                outs[3 + place][tile - FRONT] = value

        for slot in range(Q):
            for plane in range(2):
                for side in range(2):
                    put(
                        4 * slot + 2 * plane + side,
                        load(slot, plane, 2 * block + 1 + side),
                    )
        ends = []
        for plane in range(2):
            total = jnp.zeros((8, 128), F32)
            density = jnp.zeros((8, 128), F32)
            for slot in range(Q + 1):
                if slot < Q:
                    both = jnp.where(
                        lane < 64,
                        load(slot, plane, 2 * block + 3),
                        load(slot, plane, 2 * block),
                    )
                    density = density + both
                else:
                    both = density
                start, first, count = places[slot]
                moved = pltpu.roll(both, (2 + start - first) % 128, 1)
                total = jnp.where((lane >= start) & (lane < start + count), moved, total)
            ends.append(total)
        put(4 * Q, jnp.where(lane < span, ends[0], pltpu.roll(ends[1], span, 1)))


def pick_second(first, other, last, out):
    me = lax.axis_index("px")
    wanted = plan(me, me >> 2)[0]
    for k, source in enumerate((first, other, last), 1):

        @pl.when(wanted == k)
        def _():
            out[...] = source[...]


def pick_rest(*refs):
    tops, bottoms, outs = refs[:3], refs[3:6], refs[6:]
    me = lax.axis_index("px")
    for round_, wanted in enumerate(plan(me, me >> 2)):
        for k in range(1, 4):

            @pl.when(wanted == k)
            def _():
                if round_ == 0:
                    outs[0][...] = bottoms[k - 1][...]
                else:
                    outs[round_][pl.ds(0, FRONT)] = tops[k - 1][...]
                    outs[round_][pl.ds(FRONT, BACK)] = bottoms[k - 1][...]


def edge_kernel(*refs):
    nears, own, top, bottom = refs[:4], refs[4], refs[5], refs[6]
    down, up, first, last = refs[7:]
    me = lax.axis_index("px")
    half, place = me >> 2, me & 3
    for mine in range(2):
        near_to, far_to = (first, last) if mine == 0 else (last, first)
        for k in range(4):

            @pl.when((half == mine) & ((place ^ (3 * mine)) == k))
            def _():
                near_to[...] = nears[k][...]

        edge_place = 3 * (1 - mine)

        @pl.when((half == mine) & (place == edge_place))
        def _():
            far_to[...] = own[...]

        @pl.when((half == mine) & (place != edge_place))
        def _():
            far_to[pl.ds(0, FRONT)] = top[...]
            far_to[pl.ds(FRONT, BACK)] = bottom[...]

    sub = lax.broadcasted_iota(jnp.int32, (8, 128), 0)
    for out, strip, toward in ((down, first, -1), (up, last, 1)):
        near_row, far_row = (0, 1) if toward == -1 else (7, 6)
        packed = [jnp.zeros((8, 128), F32)] * HALO_TILES
        for (kind, tile), (group, row) in halo_rows(toward).items():
            if kind == "density":
                value = strip[tile]
                for slot in range(1, Q):
                    value = value + strip[4 * slot + tile]
            else:
                value = strip[tile]
            origin = near_row if kind == "near" else far_row
            packed[group] = jnp.where(sub == row, turned(value, row - origin), packed[group])
        for group in range(HALO_TILES):
            out[group] = packed[group]


def turned(value, rows):
    return pltpu.roll(value, rows % 8, 0) if rows % 8 else value


def collide(f, fluid):
    sums = [f[2 * j + 1] + f[2 * j + 2] for j in range(9)]
    diffs = [f[2 * j + 1] - f[2 * j + 2] for j in range(9)]
    density = f[0] + ((sums[0] + sums[1]) + (sums[2] + sums[3])) + (
        (sums[4] + sums[5]) + (sums[6] + sums[7]) + sums[8]
    )
    density = jnp.where(fluid, density, 1.0)
    inverse = 1.0 / density
    vel = []
    for axis in range(3):
        total = None
        for j in range(9):
            sign = lattice_velocity[2 * j + 1][axis]
            if sign:
                if total is None:
                    total = diffs[j]
                elif sign > 0:
                    total = total + diffs[j]
                else:
                    total = total - diffs[j]
        vel.append(total * inverse)
    vel[2] = vel[2] + relax_time * body_force
    speed = vel[0] * vel[0] + vel[1] * vel[1] + vel[2] * vel[2]
    rate = 1.0 / relax_time
    keep = 1.0 - rate
    scaled = density * rate
    base = scaled - 1.5 * (scaled * speed)
    out = [keep * f[0] + (1.0 / 3.0) * base]
    parts = {}
    for share in (1.0 / 18.0, 1.0 / 36.0):
        parts[share] = (share * base, share * scaled)
    for j in range(9):
        vector = lattice_velocity[2 * j + 1]
        along = None
        for axis in range(3):
            if vector[axis]:
                if along is None:
                    along = vel[axis]
                elif vector[axis] > 0:
                    along = along + vel[axis]
                else:
                    along = along - vel[axis]
        rest, weight = parts[1.0 / 18.0 if j < 3 else 1.0 / 36.0]
        tilt = weight * along
        even = rest + 4.5 * (tilt * along)
        odd = 3.0 * tilt
        out.append(keep * f[2 * j + 1] + (even + odd))
        out.append(keep * f[2 * j + 2] + (even - odd))
    return out


def rows_of(part):
    return pl.ds(pl.multiple_of(8 * part, 8), 8)


def unpack(post, read, part, outer_density=None):
    places, span = halo_lanes()
    sub = lax.broadcasted_iota(jnp.int32, (8, 128), 0)
    packed = read(4 * Q)
    for plane in range(2):
        ends = pltpu.roll(packed, 128 - span, 1) if plane else packed
        for tile in range(3):
            if tile < 2:
                values = [read(4 * slot + 2 * plane + tile) for slot in range(Q)]
                density = values[0]
                for value in values[1:]:
                    density = density + value
                if outer_density is not None:
                    density = jnp.where(
                        (sub == 1) | (sub == 6), outer_density(2 * plane + tile), density
                    )
            else:
                values = [
                    pltpu.roll(ends, (first - 2 - start) % 128, 1)
                    for start, first, _ in places
                ]
                density = values.pop()
            for slot in range(Q):
                post[slot, plane, rows_of(part), pl.ds(128 * tile, 128)] = jnp.where(
                    density > 0.0, values[slot], SOLID
                )


def streamed(array, slot, plane, part, open_here):
    sub = lax.broadcasted_iota(jnp.int32, (8, 384), 0)
    vector = lattice_velocity[slot]
    here = array[opposite[slot], plane, rows_of(part), :]
    if slot == 0:
        return jnp.where(open_here, here, 0.0)
    origin = plane if vector[2] == 0 else 1 - plane
    source = array[slot, origin, rows_of(part), :]
    if vector[1] == 1:
        beyond = array[slot, origin, rows_of(lax.rem(part + 8, 9)), :]
        source = pltpu.roll(jnp.where(sub == 7, beyond, source), 1, 0)
    elif vector[1] == -1:
        beyond = array[slot, origin, rows_of(lax.rem(part + 1, 9)), :]
        source = pltpu.roll(jnp.where(sub == 0, beyond, source), 7, 0)
    if vector[0]:
        source = pltpu.roll(source, vector[0] % 384, 1)
    return jnp.where(open_here, jnp.where(source > 0.5 * SOLID, source, here), 0.0)


def second_step(post, post2, line, part):
    for plane in range(2):
        open_here = post[0, plane, rows_of(part), :] > 0.5 * SOLID
        for slot in range(Q):
            line[slot, plane] = streamed(post, slot, plane, part, open_here)
        for tile in range(3):
            cols = pl.ds(128 * tile, 128)
            fluid = post[0, plane, rows_of(part), cols] > 0.5 * SOLID
            values = collide([line[slot, plane, :, cols] for slot in range(Q)], fluid)
            for slot in range(Q):
                post2[slot, plane, rows_of(part), cols] = jnp.where(
                    fluid, values[slot], SOLID
                )


def finish(post2, stage, flow, sem, part):
    for plane in range(2):
        open_here = post2[0, plane, rows_of(part), :] > 0.5 * SOLID
        for slot in range(Q):
            result = streamed(post2, slot, plane, part, open_here)
            stage[slot, plane, rows_of(part), :] = result[:, :256]
    part_copy(stage, flow, sem, part).start()


def part_copy(stage, flow, sem, part):
    return pltpu.make_async_copy(
        stage.at[:, :, rows_of(part), :], flow.at[:, :, rows_of(part), :], sem.at[part]
    )


def finish_start(post2, stage, flow, sem, offsets, strip):
    for offset in offsets:
        part = lax.rem(strip + offset, 9)

        @pl.when(part < 8)
        def _():
            finish(post2, stage, flow, sem, part)


def finish_wait(stage, flow, sem, offsets, strip):
    for offset in offsets:
        part = lax.rem(strip + offset, 9)

        @pl.when(part < 8)
        def _():
            part_copy(stage, flow, sem, part).wait()


def finish_all(post2, stage, flow, sem, offsets, strip):
    finish_start(post2, stage, flow, sem, offsets, strip)
    finish_wait(stage, flow, sem, offsets, strip)


def early_kernel(*refs):
    nears, own, top, bottom, third = refs[:4], refs[4], refs[5], refs[6], refs[7]
    down, up = refs[8:10]
    post, post2, flow, line, stage, sem = refs[10:]
    me = lax.axis_index("px")
    half, place = me >> 2, me & 3
    second_k, third_k, last_k = plan(me, 1 - half)
    base = 4 * (1 - half)
    for k in range(4):
        unpack(post, lambda t, k=k: nears[k][t], me ^ k)
    unpack(post, lambda t: own[t], base + place)
    unpack(
        post,
        lambda t: top[t] if t < FRONT else bottom[t - FRONT],
        base + (place ^ second_k),
    )
    unpack(post, lambda t: third[t], base + (place ^ third_k))
    sub = lax.broadcasted_iota(jnp.int32, (8, 128), 0)

    below, above = halo_rows(-1), halo_rows(1)

    def row_from(array, where, row):
        group, origin = where
        return turned(array[group], row - origin)

    def ring(tile):
        value = jnp.where(
            sub == 0,
            row_from(down, below["near", tile], 0),
            row_from(up, above["near", tile], 7),
        )
        if ("far", tile) in below:
            value = jnp.where(sub == 1, row_from(down, below["far", tile], 1), value)
        if ("far", tile) in above:
            value = jnp.where(sub == 6, row_from(up, above["far", tile], 6), value)
        return value

    def ring_density(tile):
        return jnp.where(
            sub == 1,
            row_from(down, below["density", tile], 1),
            row_from(up, above["density", tile], 6),
        )

    unpack(post, ring, 8, ring_density)
    strip = base + (place ^ last_k)

    def step(offset, carry):
        second_step(post, post2, line, lax.rem(strip + offset, 9))
        return carry

    lax.fori_loop(2, 8, step, 0)
    finish_all(post2, stage, flow, sem, (3, 4, 5, 6), strip)


def late_kernel(last, post_in, post2_in, flow_in, post, post2, flow, line, stage, sem):
    me = lax.axis_index("px")
    half, place = me >> 2, me & 3
    strip = 4 * (1 - half) + (place ^ plan(me, 1 - half)[2])
    unpack(post, lambda t: last[t], strip)

    ready = {8: (7,), 0: (8,), 1: (0, 1, 2)}
    for offset, complete in ready.items():
        second_step(post, post2, line, lax.rem(strip + offset, 9))
        finish_start(post2, stage, flow, sem, complete, strip)
    finish_wait(stage, flow, sem, (7, 8, 0, 1, 2), strip)


def tiles_of(count):
    return jax.ShapeDtypeStruct((count, 8, 128), F32)


def vmem(count):
    return [pl.BlockSpec(memory_space=pltpu.VMEM)] * count


def anywhere(count):
    return [pl.BlockSpec(memory_space=pl.ANY)] * count


def grant(mebibytes):
    return pltpu.CompilerParams(vmem_limit_bytes=mebibytes * 2**20)


def cost(flops):
    return pl.CostEstimate(flops=flops, bytes_accessed=2_000_000, transcendentals=0)


def step_pair(populations, pore):
    planes, rows, width = populations.shape[1:]
    wide = width // 2 + 256

    def call(
        kernel, shapes, operands, grant_mib, scratch=(), flops=300_000, specs=None
    ):
        return pl.pallas_call(
            kernel,
            out_shape=shapes,
            in_specs=specs or vmem(len(operands)),
            out_specs=vmem(len(shapes)),
            scratch_shapes=list(scratch),
            compiler_params=grant(grant_mib),
            cost_estimate=cost(flops),
        )(*operands)

    def pack(far):
        whole = tiles_of(TILES)
        scratch = [pltpu.VMEM((Q, planes, rows, wide), F32)]
        scratch += [
            pltpu.VMEM((Q, planes, rows, wide), F32),
            pltpu.VMEM((planes, rows, wide), jnp.int32),
            pltpu.SemaphoreType.DMA((2, 6)),
        ]
        return call(
            lambda *refs: pack_kernel(*refs, far=far),
            [whole] + [tiles_of(FRONT)] * 3 + [tiles_of(BACK)] * 3 if far else [whole] * 4,
            (populations, pore),
            52,
            scratch=scratch,
            flops=4_000_000,
            specs=anywhere(2),
        )

    def trade(array, k):
        return lax.ppermute(array, "px", [(i, i ^ k) for i in range(8)])

    far = pack(1)
    near = pack(0)
    own = trade(far[0], 4)
    tops = [trade(far[k], k) for k in range(1, 4)]
    bottoms = [trade(far[3 + k], k) for k in range(1, 4)]
    (second,) = call(pick_second, [tiles_of(FRONT)], tops, 2)
    rest = call(
        pick_rest, [tiles_of(BACK), tiles_of(TILES), tiles_of(TILES)], tops + bottoms, 4
    )
    second_top = trade(second, 4)
    nears = [near[0]] + [trade(near[k], k) for k in range(1, 4)]
    second_bottom = trade(rest[0], 4)
    third = trade(rest[1], 4)
    fourth = trade(rest[2], 4)

    arrived = nears + [own, second_top, second_bottom]
    down, up = call(
        edge_kernel,
        [tiles_of(HALO_TILES)] * 2,
        arrived,
        4,
        scratch=[pltpu.VMEM((TILES, 8, 128), F32)] * 2,
        flops=500_000,
    )
    count = lax.axis_size("py")
    down = lax.ppermute(down, "py", [((i + 1) % count, i) for i in range(count)])
    up = lax.ppermute(up, "py", [(i, (i + 1) % count) for i in range(count)])

    ring = jax.ShapeDtypeStruct((Q, planes, 72, 384), F32)
    result = jax.ShapeDtypeStruct((Q, planes, 64, 256), F32)
    scratch = [
        pltpu.VMEM((Q, planes, 8, 384), F32),
        pltpu.VMEM((Q, planes, 64, 256), F32),
        pltpu.SemaphoreType.DMA((9,)),
    ]
    post, post2, flow = pl.pallas_call(
        early_kernel,
        out_shape=[ring, ring, result],
        in_specs=vmem(10),
        out_specs=vmem(2) + anywhere(1),
        scratch_shapes=scratch,
        compiler_params=grant(24),
        cost_estimate=cost(40_000_000),
        name="early",
    )(*arrived, third, down, up)
    return pl.pallas_call(
        late_kernel,
        out_shape=[ring, ring, result],
        in_specs=vmem(3) + anywhere(1),
        out_specs=vmem(2) + anywhere(1),
        scratch_shapes=scratch,
        input_output_aliases={1: 0, 2: 1, 3: 2},
        compiler_params=grant(24),
        cost_estimate=cost(10_000_000),
        name="late",
    )(fourth, post, post2, flow)[2]


def solution(mesh):
    return jax.shard_map(
        step_pair,
        mesh=mesh,
        in_specs=(P(None, None, ("py", "px"), None), P(None, ("py", "px"), None)),
        out_specs=P(None, None, "py", "px"),
        check_vma=False,
    )
```
